32 devices in a mesh: lon: 16 (over z, y, core), lat: 2 (over x).
Axes of the slice: x: 2, y: 2, z: 4, core: 2. Of those that a mesh axis runs over, the one named last changes fastest.
Arguments:
- fields: bfloat16 [256, 512, 256], P('lat', 'lon'), may hold values from -6 to 6
- spec_weight: bfloat16 [2, 2, 17, 256, 256], replicated, may hold values from -0.75 to 0.75
- skip_weight: bfloat16 [2, 256, 256], replicated, may hold values from -0.375 to 0.375
- diffusion: float32 [2, 256], replicated, may hold values from 0.2 to 1
Outputs:
- result: bfloat16 [256, 512, 256], P('lat', 'lon')
The draws below stay inside these ranges and needn't reach their ends.
All inputs are finite; a program needn't handle non-finite values.
Results may differ from the reference program's by a relative error of at most 0.01.
Values may be sent and summed in bfloat16 or wider, within the bound.
A program may use at most 128 MiB of HBM per device.

```python
import math
import jax
import jax.numpy as jnp
from jax import lax

C = 256
WINDOW = 64
HOP = 32
MODES = 17
LAYERS = 2
LAT_DEV = 128
NLAT = 256
NLON = 512
N_LAT = 2


def level_of(stream_key, extent, shards, low, largest):
    def one(dim, blocks):
        heights = jax.random.uniform(jax.random.fold_in(jax.random.fold_in(stream_key, 6), dim), (blocks,), jnp.float32, low / len(shards), largest / len(shards))
        return jnp.repeat(jnp.exp(heights), extent[dim] // blocks).reshape((-1,) + (1,) * (len(extent) - dim - 1))

    gain = one(*shards[0])
    for cut in shards[1:]:
        gain = gain * one(*cut)
    return gain


def gaussian(own_key, shape, deviation, most, cuts=(), kind=jnp.bfloat16):
    entries = jax.random.normal(own_key, shape, jnp.float32) * deviation
    if len(cuts) > 0:
        entries = level_of(own_key, shape, cuts, -0.22, 0.18) * entries
    return jnp.clip(entries, min=-most, max=most).astype(kind)


def setup_inputs(seed: int = 0) -> dict:
    key_list = jax.random.split(jax.random.key(seed), 5)
    fields = gaussian(key_list[0], (NLAT, NLON, C), 1.0, 6.0, ((0, 2), (1, 16)))
    spec_weight = gaussian(key_list[1], (LAYERS, 2, MODES, C, C), (C // 4) ** -0.5, 0.75)
    skip_weight = gaussian(key_list[2], (LAYERS, C, C), C ** -0.5, 0.375)
    diffusion = jnp.clip(jnp.exp(jax.random.uniform(key_list[3], (LAYERS, C), jnp.float32, math.log(0.2), math.log(1.0))), 0.2, 1.0)
    return dict(fields=fields, spec_weight=spec_weight, skip_weight=skip_weight, diffusion=diffusion)


def tables(window, mode_count):
    points = jnp.arange(window, dtype=jnp.float32)
    freqs = jnp.arange(mode_count, dtype=jnp.float32)
    angles = 2.0 * math.pi * points[:, None] * freqs[None, :] / window
    taper = 0.5 - 0.5 * jnp.cos(2.0 * math.pi * points / window)
    analysis = jnp.concatenate([taper[:, None] * jnp.cos(angles), -taper[:, None] * jnp.sin(angles)], axis=1).astype(jnp.bfloat16)
    factor = jnp.where(freqs == 0.0, 1.0, 2.0) / window
    synthesis = jnp.concatenate([factor[:, None] * jnp.cos(angles).T, -factor[:, None] * jnp.sin(angles).T], axis=0).astype(jnp.bfloat16)
    return analysis, synthesis


def transform_frames(halves, spec_weight, analysis, synthesis, hop, mode_count):
    halves_wide = halves.astype(jnp.float32)
    front_part = jnp.einsum('lhnc,nj->lhjc', halves_wide, analysis[:hop].astype(jnp.float32))
    back_part = jnp.einsum('lhnc,nj->lhjc', halves_wide, analysis[hop:].astype(jnp.float32))
    coeffs = (front_part[:, :-1] + back_part[:, 1:]).astype(jnp.bfloat16).astype(jnp.float32)
    real_part = coeffs[:, :, :mode_count]
    imag_part = coeffs[:, :, mode_count:]
    weight_real = spec_weight[0].astype(jnp.float32)
    weight_imag = spec_weight[1].astype(jnp.float32)
    mix_real = jnp.einsum('lfkc,kcd->lfkd', real_part, weight_real) - jnp.einsum('lfkc,kcd->lfkd', imag_part, weight_imag)
    mix_imag = jnp.einsum('lfkc,kcd->lfkd', real_part, weight_imag) + jnp.einsum('lfkc,kcd->lfkd', imag_part, weight_real)
    mixed = jnp.concatenate([mix_real, mix_imag], axis=2).astype(jnp.bfloat16).astype(jnp.float32)
    frames_out = jnp.einsum('jn,lfjd->lfnd', synthesis.astype(jnp.float32), mixed)
    return frames_out[:, :, :hop], frames_out[:, :, hop:]


def one_layer(state, layer_spec, layer_skip, layer_diff, analysis, synthesis):
    padded = jnp.pad(state, ((1, 1), (0, 0), (0, 0)))
    frame_count = NLON // HOP

    def band(block):
        start = (block * LAT_DEV).astype(jnp.int32)
        bordered = lax.dynamic_slice_in_dim(padded, start, LAT_DEV + 2, 0)
        centre = bordered[1:-1]
        extended = jnp.concatenate([centre, centre[:, :HOP]], axis=1)
        halves = extended.reshape(LAT_DEV, frame_count + 1, HOP, C)
        first_half, second_half = transform_frames(halves, layer_spec, analysis, synthesis, HOP, MODES)
        spectral = (first_half + jnp.roll(second_half, 1, axis=1)).reshape(LAT_DEV, NLON, C)
        centre_wide = centre.astype(jnp.float32)
        laplacian = bordered[2:].astype(jnp.float32) + bordered[:-2].astype(jnp.float32) - 2.0 * centre_wide
        skipped = jnp.einsum('lwc,cd->lwd', centre_wide, layer_skip.astype(jnp.float32))
        local_term = skipped + layer_diff.astype(jnp.float32) * laplacian
        hidden = spectral + local_term
        return (centre_wide + jax.nn.gelu(hidden)).astype(jnp.bfloat16)

    blocks = lax.map(band, jnp.arange(N_LAT, dtype=jnp.int32))
    return blocks.reshape(NLAT, NLON, C)


def reference(fields, spec_weight, skip_weight, diffusion):
    analysis, synthesis = tables(WINDOW, MODES)
    state = fields
    for layer in range(LAYERS):
        state = one_layer(state, spec_weight[layer], skip_weight[layer], diffusion[layer], analysis, synthesis)
    return state
```

```python
import functools

import jax
import jax.numpy as jnp
import ml_dtypes
import numpy as np
from jax import lax
from jax.experimental import pallas as pl
from jax.experimental.pallas import tpu as pltpu
from jax.sharding import PartitionSpec as P

WINDOW = 64
HOP = 32
MODES = 17
LAYERS = 2
GROUP = 4
STRIPS = 2 * GROUP
COEFS = 2 * MODES
CHUNKS = 2


def tables():
    points = np.arange(WINDOW, dtype=np.float64)
    freqs = np.arange(MODES, dtype=np.float64)
    angles = 2.0 * np.pi * points[:, None] * freqs[None, :] / WINDOW
    taper = 0.5 - 0.5 * np.cos(2.0 * np.pi * points / WINDOW)
    analysis = np.concatenate(
        [taper[:, None] * np.cos(angles), -taper[:, None] * np.sin(angles)], axis=1
    )
    factor = np.where(freqs == 0.0, 1.0, 2.0) / WINDOW
    synthesis = np.concatenate(
        [factor[:, None] * np.cos(angles).T, -factor[:, None] * np.sin(angles).T], axis=0
    )
    return analysis, synthesis


def banded_tables():
    analysis, synthesis = tables()
    length = STRIPS * HOP
    forward = np.zeros((COEFS, STRIPS, length))
    backward = np.zeros((length, COEFS, STRIPS))
    for f in range(STRIPS):
        cells = (f * HOP + np.arange(WINDOW)) % length
        forward[:, f, cells] = analysis.T
        backward[cells, :, f] = synthesis.T
    kind = ml_dtypes.bfloat16
    forward = forward.reshape(COEFS * STRIPS, length).astype(np.float32).astype(kind)
    backward = backward.reshape(length, COEFS * STRIPS).astype(np.float32).astype(kind)
    return forward, backward


def gelu(x):
    return jax.nn.gelu(x, approximate=True)


def layer_rows(rows, source, source_lo, target, lo, hi, forward, backward, spec, skip, diff, coefs, valid):
    channels = skip.shape[-1]
    pairs = rows // 2

    def analyse(pair, carry):
        parts = []
        for half in range(2):
            x = source[2 * pair + half + 1]
            part = jnp.dot(forward[...], x, preferred_element_type=jnp.float32)
            parts.append(part.reshape(COEFS, STRIPS, channels))
        both = jnp.concatenate(parts, axis=1).astype(jnp.bfloat16)
        coefs[:, pl.ds(pl.multiple_of(pair * 2 * STRIPS, 2 * STRIPS), 2 * STRIPS), :] = both
        return carry

    lax.fori_loop(0, pairs, analyse, 0)

    used = rows * STRIPS

    def mix(k, carry):
        real = coefs[k, :used]
        imag = coefs[MODES + k, :used]
        weight_real = spec[0, k]
        weight_imag = spec[1, k]
        dot = functools.partial(jnp.dot, preferred_element_type=jnp.float32)
        mixed_real = dot(real, weight_real) - dot(imag, weight_imag)
        mixed_imag = dot(real, weight_imag) + dot(imag, weight_real)
        coefs[k, :used] = mixed_real.astype(jnp.bfloat16)
        coefs[MODES + k, :used] = mixed_imag.astype(jnp.bfloat16)
        return carry

    lax.fori_loop(0, MODES, mix, 0)

    def synthesise(pair, carry):
        both = coefs[:, pl.ds(pl.multiple_of(pair * 2 * STRIPS, 2 * STRIPS), 2 * STRIPS), :].astype(jnp.float32)
        for half in range(2):
            row = 2 * pair + half
            mixed = both[:, half * STRIPS : (half + 1) * STRIPS]
            mixed = mixed.reshape(COEFS * STRIPS, channels).astype(jnp.bfloat16)
            cells = pl.ds(lo - source_lo, hi - lo)
            centre = source[row + 1, cells]
            hidden = jnp.dot(backward[lo:hi], mixed, preferred_element_type=jnp.float32)
            hidden = hidden + jnp.dot(centre, skip[...], preferred_element_type=jnp.float32)
            wide = centre.astype(jnp.float32)
            laplacian = (
                source[row + 2, cells].astype(jnp.float32) + source[row, cells].astype(jnp.float32) - 2.0 * wide
            )
            hidden = hidden + diff * laplacian
            result = wide + gelu(hidden)
            if valid is not None:
                result = jnp.where(valid(row), result, 0.0)
            target[row] = result.astype(jnp.bfloat16)
        return carry

    lax.fori_loop(0, pairs, synthesise, 0)


def kernel(
    chunk, out_rows, group_rows, band_rows, grid_rows, has_tail,
    *refs,
):
    count = 6 if not has_tail else 12
    pieces = refs[:count]
    spec_hbm, skip, diffusion, forward, forward_inner, backward = refs[count : count + 6]
    outs = refs[count + 6 : count + 6 + GROUP]
    window, middle, final, coefs, spec, in_sems, spec_sems, out_sems = refs[count + 6 + GROUP :]
    place = lax.rem(lax.axis_index("lon"), GROUP)

    loads = []
    for layer in range(LAYERS):
        copy = pltpu.make_async_copy(spec_hbm.at[layer], spec.at[layer], spec_sems.at[layer])
        copy.start()
        loads.append(copy)

    def xor(d):
        low = lax.rem(place, 2)
        high = place // 2
        low = 1 - low if d & 1 else low
        high = 1 - high if d & 2 else high
        return 2 * high + low

    copies = []

    def load(piece, first, number, at, strip):
        copy = pltpu.make_async_copy(
            piece.at[pl.ds(first, number)],
            window.at[pl.ds(at, number), pl.ds(pl.multiple_of(strip * HOP, HOP), HOP)],
            in_sems.at[len(copies)],
        )
        copy.start()
        copies.append(copy)

    def load_set(six, first, number, at):
        for d in range(GROUP):
            load(six[d], first, number, at, xor(d) + 2)
        for d in range(2):
            parity = lax.rem(xor(d), 2)
            load(six[4].at[d], first, number, at, parity)
            load(six[5].at[d], first, number, at, parity + 6)

    if has_tail:
        length = pieces[0].shape[0]
        load_set(pieces[:6], length - 4, 4, 0)
        load_set(pieces[6:], 0, out_rows, 4)
    else:
        load_set(pieces, 0, out_rows + 4, 0)
    for copy in copies:
        copy.wait()

    base = lax.axis_index("lat") * band_rows + place * group_rows + chunk * out_rows - 1

    def valid(row):
        at = base + row
        return jnp.logical_and(at >= 0, at < grid_rows)

    length = STRIPS * HOP
    loads[0].wait()
    layer_rows(
        out_rows + 2, window, 0, middle, HOP, length - HOP, forward, backward,
        spec.at[0], skip.at[0], diffusion[0:1], coefs, valid,
    )
    loads[1].wait()
    layer_rows(
        out_rows, middle, HOP, final, 2 * HOP, length - 2 * HOP, forward_inner, backward,
        spec.at[1], skip.at[1], diffusion[1:2], coefs, None,
    )
    stores = []
    for d in range(GROUP):
        copy = pltpu.make_async_copy(
            final.at[:, pl.ds(pl.multiple_of(xor(d) * HOP, HOP), HOP)], outs[d], out_sems.at[d]
        )
        copy.start()
        stores.append(copy)
    for copy in stores:
        copy.wait()


def compute(chunk, pieces, has_tail, out_rows, group_rows, band_rows, grid_rows, spec, skip, diffusion, consts):
    channels = skip.shape[-1]
    length = STRIPS * HOP
    anywhere = pl.BlockSpec(memory_space=pl.ANY)
    inside = pl.BlockSpec(memory_space=pltpu.VMEM)
    rows = 2 * out_rows + 2
    macs = rows * STRIPS * channels * (COEFS * 2 * channels + 2 * COEFS * WINDOW * 4 + HOP * channels)
    return pl.pallas_call(
        functools.partial(kernel, chunk, out_rows, group_rows, band_rows, grid_rows, has_tail),
        out_shape=[jax.ShapeDtypeStruct((out_rows, HOP, channels), jnp.bfloat16)] * GROUP,
        in_specs=[anywhere] * (len(pieces) + 1) + [inside] * 5,
        out_specs=[anywhere] * GROUP,
        scratch_shapes=[
            pltpu.VMEM((out_rows + 4, length, channels), jnp.bfloat16),
            pltpu.VMEM((out_rows + 2, length - 2 * HOP, channels), jnp.bfloat16),
            pltpu.VMEM((out_rows, length - 4 * HOP, channels), jnp.bfloat16),
            pltpu.VMEM((COEFS, (out_rows + 2) * STRIPS, channels), jnp.bfloat16),
            pltpu.VMEM(spec.shape, jnp.bfloat16),
            pltpu.SemaphoreType.DMA((16,)),
            pltpu.SemaphoreType.DMA((LAYERS,)),
            pltpu.SemaphoreType.DMA((GROUP,)),
        ],
        compiler_params=pltpu.CompilerParams(vmem_limit_bytes=56 * 1024 * 1024),
        cost_estimate=pl.CostEstimate(
            flops=2 * macs, bytes_accessed=2 * spec.size, transcendentals=rows * length * channels
        ),
    )(*pieces, spec, skip, diffusion, *consts)


def local(grid_rows, fields, spec_weight, skip_weight, diffusion):
    band_rows, strip, channels = fields.shape
    count = lax.axis_size("lon")
    lats = lax.axis_size("lat")
    group_rows = band_rows // GROUP
    out_rows = group_rows // CHUNKS
    place = lax.axis_index("lon") % GROUP
    forward, backward = banded_tables()
    consts = (jnp.asarray(forward), jnp.asarray(forward[:, HOP:-HOP]), jnp.asarray(backward))

    above = lax.ppermute(fields[-2:], "lat", [(i, i + 1) for i in range(lats - 1)])
    below = lax.ppermute(fields[:2], "lat", [(i + 1, i) for i in range(lats - 1)])
    bordered = jnp.concatenate([above, fields, below], axis=0)

    def swap(x, d):
        return lax.ppermute(x, "lon", [(i, i ^ d) for i in range(count)])

    def around(x, by):
        return lax.ppermute(x, "lon", [(i, (i + by) % count) for i in range(count)])

    upper = place >= 2
    sets = []
    for chunk in range(CHUNKS):
        first = 0 if chunk == 0 else chunk * out_rows + 4
        number = out_rows + 4 if chunk == 0 else out_rows
        got = []
        for d in range(GROUP):
            piece = lax.dynamic_slice_in_dim(bordered, (place ^ d) * group_rows + first, number, 0)
            got.append(piece if d == 0 else swap(piece, d))
        own = jnp.stack(got[:2])
        other = jnp.stack(got[2:])
        right = around(jnp.where(upper, other, own), -GROUP)
        left = around(jnp.where(upper, own, other), GROUP)
        sets.append(got + [left, right])

    result = jnp.zeros_like(fields)
    for chunk in range(CHUNKS):
        tail = [] if chunk == 0 else [t for t in sets[chunk - 1]]
        if chunk:
            tail = [t[-4:] if t.ndim == 3 else t[:, -4:] for t in tail]
        outs = compute(
            chunk, tail + sets[chunk], chunk > 0, out_rows, group_rows, band_rows, grid_rows,
            spec_weight, skip_weight, diffusion, consts,
        )
        for d in range(GROUP):
            back = outs[d] if d == 0 else swap(outs[d], d)
            result = lax.dynamic_update_slice_in_dim(
                result, back, (place ^ d) * group_rows + chunk * out_rows, 0
            )
    return result


def solution(mesh):
    in_specs = (P("lat", "lon", None), P(), P(), P())
    out_specs = P("lat", "lon", None)

    def whole(fields, spec_weight, skip_weight, diffusion):
        step = functools.partial(local, fields.shape[0])
        return jax.shard_map(step, mesh=mesh, in_specs=in_specs, out_specs=out_specs, check_vma=False)(
            fields, spec_weight, skip_weight, diffusion
        )

    return whole
```

```python
import functools

import jax
import jax.numpy as jnp
import ml_dtypes
import numpy as np
from jax import lax
from jax.experimental import pallas as pl
from jax.experimental.pallas import tpu as pltpu
from jax.sharding import PartitionSpec as P

WINDOW = 64
HOP = 32
MODES = 17
LAYERS = 2
GROUP = 4
STRIPS = 2 * GROUP
COEFS = 2 * MODES
CHUNKS = 4

def tables():
    points = np.arange(WINDOW, dtype=np.float64)
    freqs = np.arange(MODES, dtype=np.float64)
    angles = 2.0 * np.pi * points[:, None] * freqs[None, :] / WINDOW
    taper = 0.5 - 0.5 * np.cos(2.0 * np.pi * points / WINDOW)
    analysis = np.concatenate(
        [taper[:, None] * np.cos(angles), -taper[:, None] * np.sin(angles)], axis=1
    )
    factor = np.where(freqs == 0.0, 1.0, 2.0) / WINDOW
    synthesis = np.concatenate(
        [factor[:, None] * np.cos(angles).T, -factor[:, None] * np.sin(angles).T], axis=0
    )
    return analysis, synthesis


def banded_tables():
    analysis, synthesis = tables()
    length = STRIPS * HOP
    forward = np.zeros((COEFS, STRIPS, length))
    backward = np.zeros((length, COEFS, STRIPS))
    for f in range(STRIPS):
        cells = (f * HOP + np.arange(WINDOW)) % length
        forward[:, f, cells] = analysis.T
        backward[cells, :, f] = synthesis.T
    kind = ml_dtypes.bfloat16
    forward = forward.reshape(COEFS * STRIPS, length).astype(np.float32).astype(kind)
    backward = backward.reshape(length, COEFS * STRIPS).astype(np.float32).astype(kind)
    return forward, backward


def gelu(x):
    return jax.nn.gelu(x, approximate=True)


def layer_rows(rows, first, source, source_lo, target, target_first, lo, hi, forward, backward, spec, skip, diff, coefs, valid):
    channels = skip.shape[-1]
    pairs = rows // 2

    def analyse(pair, carry):
        parts = []
        for half in range(2):
            x = source[first + 2 * pair + half + 1]
            part = jnp.dot(forward[...], x, preferred_element_type=jnp.float32)
            parts.append(part.reshape(COEFS, STRIPS, channels))
        both = jnp.concatenate(parts, axis=1).astype(jnp.bfloat16)
        coefs[:, pl.ds(pl.multiple_of(pair * 2 * STRIPS, 2 * STRIPS), 2 * STRIPS), :] = both
        return carry

    lax.fori_loop(0, pairs, analyse, 0)

    used = rows * STRIPS

    def mix(k, carry):
        real = coefs[k, :used]
        imag = coefs[MODES + k, :used]
        weight_real = spec[0, k]
        weight_imag = spec[1, k]
        dot = functools.partial(jnp.dot, preferred_element_type=jnp.float32)
        mixed_real = dot(real, weight_real) - dot(imag, weight_imag)
        mixed_imag = dot(real, weight_imag) + dot(imag, weight_real)
        coefs[k, :used] = mixed_real.astype(jnp.bfloat16)
        coefs[MODES + k, :used] = mixed_imag.astype(jnp.bfloat16)
        return carry

    lax.fori_loop(0, MODES, mix, 0)

    def synthesise(pair, carry):
        both = coefs[:, pl.ds(pl.multiple_of(pair * 2 * STRIPS, 2 * STRIPS), 2 * STRIPS), :].astype(jnp.float32)
        for half in range(2):
            row = 2 * pair + half
            mixed = both[:, half * STRIPS : (half + 1) * STRIPS]
            mixed = mixed.reshape(COEFS * STRIPS, channels).astype(jnp.bfloat16)
            cells = pl.ds(lo - source_lo, hi - lo)
            centre = source[first + row + 1, cells]
            hidden = jnp.dot(backward[lo:hi], mixed, preferred_element_type=jnp.float32)
            hidden = hidden + jnp.dot(centre, skip[...], preferred_element_type=jnp.float32)
            wide = centre.astype(jnp.float32)
            laplacian = (
                source[first + row + 2, cells].astype(jnp.float32) + source[first + row, cells].astype(jnp.float32) - 2.0 * wide
            )
            hidden = hidden + diff * laplacian
            result = wide + gelu(hidden)
            if valid is not None:
                result = jnp.where(valid(row), result, 0.0)
            target[target_first + row] = result.astype(jnp.bfloat16)
        return carry

    lax.fori_loop(0, pairs, synthesise, 0)


def kernel(
    group_rows, band_rows, grid_rows, count, lats,
    padded, spec_hbm, skip, diffusion, forward, forward_inner, backward,
    result,
    window, middle, final, coefs, spec, edges,
    spec_sems, own_sems, put_sems, y_send, y_recv, z_send, z_recv, lat_send, lat_recv, out_send, out_recv,
):
    index = lax.axis_index("lon")
    lat = lax.axis_index("lat")
    place = lax.rem(index, GROUP)
    base = index - place
    quarter = group_rows // CHUNKS
    length = STRIPS * HOP
    pieces = [
        (quarter, quarter + 4),
        (2 * quarter + 4, quarter),
        (0, quarter),
        (3 * quarter + 4, quarter),
    ]
    upward = lax.rem(index + GROUP, count)
    downward = lax.rem(index + count - GROUP, count)

    def xor(d):
        low = lax.rem(place, 2)
        high = place // 2
        low = 1 - low if d & 1 else low
        high = 1 - high if d & 2 else high
        return 2 * high + low

    def strip(at):
        return pl.ds(pl.multiple_of((at + 2) * HOP, HOP), HOP)

    def remote(source, target, send, recv, where):
        return pltpu.make_async_remote_copy(
            src_ref=source, dst_ref=target, send_sem=send, recv_sem=recv,
            device_id=where, device_id_type=pl.DeviceIdType.MESH,
        )

    def y_copy(n, d, receive):
        first, number = pieces[n]
        other = xor(d)
        owner = other if receive else place
        return remote(
            padded.at[pl.ds(other * group_rows + first, number)],
            window.at[pl.ds(first, number), strip(owner)],
            y_send.at[n, d], y_recv.at[n, d], {"lon": base + other},
        )

    def z_copy(n, side, receive):
        first, number = pieces[n]
        rows = pl.ds(first, number)
        if side == 0:
            source, target, where = 4 * HOP, 0, upward
        else:
            source, target, where = 2 * HOP, 6 * HOP, downward
        return remote(
            window.at[rows, pl.ds(source, 2 * HOP)],
            window.at[rows, pl.ds(target, 2 * HOP)],
            z_send.at[n, side], z_recv.at[n, side], {"lon": where},
        )

    def out_copy(chunk, d, receive):
        other = xor(d)
        owner = other if receive else place
        return remote(
            final.at[pl.ds(chunk * quarter, quarter), pl.ds(pl.multiple_of(other * HOP, HOP), HOP)],
            result.at[pl.ds(owner * group_rows + chunk * quarter, quarter)],
            out_send.at[chunk, d], out_recv.at[chunk, d], {"lon": base + other},
        )

    own = []
    for n in range(CHUNKS):
        first, number = pieces[n]
        for d in (2, 3, 1):
            y_copy(n, d, False).start()
        copy = pltpu.make_async_copy(
            padded.at[pl.ds(place * group_rows + first, number)],
            window.at[pl.ds(first, number), strip(place)],
            own_sems.at[n],
        )
        copy.start()
        own.append(copy)
    loads = []
    for layer in range(LAYERS):
        copy = pltpu.make_async_copy(spec_hbm.at[layer], spec.at[layer], spec_sems.at[layer])
        copy.start()
        loads.append(copy)

    for n in range(CHUNKS):
        own[n].wait()
        for d in (1, 2, 3):
            y_copy(n, d, True).wait_recv()
        for side in range(2):
            z_copy(n, side, False).start()

    low_edge = jnp.logical_and(place == 0, lat > 0)
    high_edge = jnp.logical_and(place == GROUP - 1, lat < lats - 1)

    def to_before():
        return remote(
            window.at[pl.ds(2, 2)], edges.at[1], lat_send.at[0], lat_recv.at[1],
            {"lon": base + GROUP - 1, "lat": jnp.maximum(lat - 1, 0)},
        )

    def to_after():
        return remote(
            window.at[pl.ds(group_rows, 2)], edges.at[0], lat_send.at[1], lat_recv.at[0],
            {"lon": base, "lat": jnp.minimum(lat + 1, lats - 1)},
        )

    def run(chunk):
        start = chunk * quarter
        top = lat * band_rows + place * group_rows + start - 1

        def valid(row):
            at = top + row
            return jnp.logical_and(at >= 0, at < grid_rows)

        layer_rows(
            quarter + 2, start, window, 0, middle, 0, HOP, length - HOP, forward, backward,
            spec.at[0], skip.at[0], diffusion[0:1], coefs, valid,
        )
        layer_rows(
            quarter, 0, middle, HOP, final, start, 2 * HOP, length - 2 * HOP, forward_inner, backward,
            spec.at[1], skip.at[1], diffusion[1:2], coefs, None,
        )
        for d in (2, 3, 1):
            out_copy(chunk, d, False).start()
        put = pltpu.make_async_copy(
            final.at[pl.ds(start, quarter), pl.ds(pl.multiple_of(place * HOP, HOP), HOP)],
            result.at[pl.ds(place * group_rows + start, quarter)],
            put_sems.at[chunk],
        )
        put.start()
        return put

    def arrived(n):
        for side in range(2):
            z_copy(n, side, True).wait_recv()
            z_copy(n, side, False).wait_send()

    puts = []
    arrived(0)
    for copy in loads:
        copy.wait()
    puts.append(run(1))
    arrived(1)
    puts.append(run(2))
    arrived(2)

    @pl.when(low_edge)
    def _():
        to_before().start()

    arrived(3)

    @pl.when(high_edge)
    def _():
        to_after().start()
        to_before().wait_recv()
        window[group_rows + 2 : group_rows + 4] = edges[1]

    puts.append(run(3))

    @pl.when(low_edge)
    def _():
        to_after().wait_recv()
        window[0:2] = edges[0]

    puts.append(run(0))

    for put in puts:
        put.wait()

    @pl.when(low_edge)
    def _():
        to_before().wait_send()

    @pl.when(high_edge)
    def _():
        to_after().wait_send()

    for n in range(CHUNKS):
        for d in (1, 2, 3):
            y_copy(n, d, False).wait_send()
            out_copy(n, d, False).wait_send()
    for n in range(CHUNKS):
        for d in (1, 2, 3):
            out_copy(n, d, True).wait_recv()


def local(grid_rows, fields, spec_weight, skip_weight, diffusion):
    band_rows, strip, channels = fields.shape
    group_rows = band_rows // GROUP
    quarter = group_rows // CHUNKS
    length = STRIPS * HOP
    forward, backward = banded_tables()
    consts = (jnp.asarray(forward), jnp.asarray(forward[:, HOP:-HOP]), jnp.asarray(backward))
    padded = jnp.pad(fields, ((2, 2), (0, 0), (0, 0)))
    anywhere = pl.BlockSpec(memory_space=pl.ANY)
    inside = pl.BlockSpec(memory_space=pltpu.VMEM)
    dma = pltpu.SemaphoreType.DMA
    return pl.pallas_call(
        functools.partial(
            kernel, group_rows, band_rows, grid_rows, lax.axis_size("lon"), lax.axis_size("lat")
        ),
        out_shape=jax.ShapeDtypeStruct(fields.shape, jnp.bfloat16),
        in_specs=[anywhere] * 2 + [inside] * 5,
        out_specs=anywhere,
        scratch_shapes=[
            pltpu.VMEM((group_rows + 4, length, channels), jnp.bfloat16),
            pltpu.VMEM((quarter + 2, length - 2 * HOP, channels), jnp.bfloat16),
            pltpu.VMEM((group_rows, length - 4 * HOP, channels), jnp.bfloat16),
            pltpu.VMEM((COEFS, (quarter + 2) * STRIPS, channels), jnp.bfloat16),
            pltpu.VMEM(spec_weight.shape, jnp.bfloat16),
            pltpu.VMEM((2, 2, length, channels), jnp.bfloat16),
            dma((LAYERS,)), dma((CHUNKS,)), dma((CHUNKS,)),
            dma((CHUNKS, GROUP)), dma((CHUNKS, GROUP)),
            dma((CHUNKS, 2)), dma((CHUNKS, 2)),
            dma((2,)), dma((2,)),
            dma((CHUNKS, GROUP)), dma((CHUNKS, GROUP)),
        ],
        compiler_params=pltpu.CompilerParams(
            vmem_limit_bytes=56 * 1024 * 1024, has_side_effects=True
        ),
    )(padded, spec_weight, skip_weight, diffusion, *consts)


def solution(mesh):
    in_specs = (P("lat", "lon", None), P(), P(), P())
    out_specs = P("lat", "lon", None)

    def whole(fields, spec_weight, skip_weight, diffusion):
        step = functools.partial(local, fields.shape[0])
        return jax.shard_map(step, mesh=mesh, in_specs=in_specs, out_specs=out_specs, check_vma=False)(
            fields, spec_weight, skip_weight, diffusion
        )

    return whole
```

```python
import functools

import jax
import jax.numpy as jnp
import ml_dtypes
import numpy as np
from jax import lax
from jax.experimental import pallas as pl
from jax.experimental.pallas import tpu as pltpu
from jax.sharding import PartitionSpec as P

WINDOW = 64
HOP = 32
MODES = 17
LAYERS = 2
GROUP = 4
STRIPS = 2 * GROUP
COEFS = 2 * MODES
CHUNKS = 4
UNROLL = 17

def tables():
    points = np.arange(WINDOW, dtype=np.float64)
    freqs = np.arange(MODES, dtype=np.float64)
    angles = 2.0 * np.pi * points[:, None] * freqs[None, :] / WINDOW
    taper = 0.5 - 0.5 * np.cos(2.0 * np.pi * points / WINDOW)
    analysis = np.concatenate(
        [taper[:, None] * np.cos(angles), -taper[:, None] * np.sin(angles)], axis=1
    )
    factor = np.where(freqs == 0.0, 1.0, 2.0) / WINDOW
    synthesis = np.concatenate(
        [factor[:, None] * np.cos(angles).T, -factor[:, None] * np.sin(angles).T], axis=0
    )
    return analysis, synthesis


def banded_tables():
    analysis, synthesis = tables()
    length = STRIPS * HOP
    forward = np.zeros((COEFS, STRIPS, length))
    backward = np.zeros((length, COEFS, STRIPS))
    for f in range(STRIPS):
        cells = (f * HOP + np.arange(WINDOW)) % length
        forward[:, f, cells] = analysis.T
        backward[cells, :, f] = synthesis.T
    kind = ml_dtypes.bfloat16
    forward = forward.reshape(COEFS * STRIPS, length).astype(np.float32).astype(kind)
    backward = backward.reshape(length, COEFS * STRIPS).astype(np.float32).astype(kind)
    return forward, backward


def gelu(x):
    return jax.nn.gelu(x, approximate=True)


def layer_rows(rows, first, source, source_lo, target, target_first, lo, hi, forward, backward, spec, skip, diff, coefs, valid):
    channels = skip.shape[-1]
    pairs = rows // 2

    def analyse(pair, carry):
        parts = []
        for half in range(2):
            x = source[first + 2 * pair + half + 1]
            part = jnp.dot(forward[...], x, preferred_element_type=jnp.float32)
            parts.append(part.reshape(COEFS, STRIPS, channels))
        both = jnp.concatenate(parts, axis=1).astype(jnp.bfloat16)
        coefs[:, pl.ds(pair * 2 * STRIPS, 2 * STRIPS), :] = both
        return carry

    for pair in range(pairs):
        analyse(pair, None)

    used = rows * STRIPS

    def mix(k, carry):
        real = coefs[k, :used]
        imag = coefs[MODES + k, :used]
        weights = jnp.concatenate([spec[0, k], spec[1, k]], axis=0)
        both = jnp.concatenate(
            [jnp.concatenate([real, -imag], axis=1), jnp.concatenate([imag, real], axis=1)], axis=0
        )
        mixed = jnp.dot(both, weights, preferred_element_type=jnp.float32).astype(jnp.bfloat16)
        coefs[k, :used] = mixed[:used]
        coefs[MODES + k, :used] = mixed[used:]

    def mix_some(step, carry):
        for k in range(UNROLL):
            mix(step * UNROLL + k, None)
        return carry

    lax.fori_loop(0, MODES // UNROLL, mix_some, 0)
    for k in range(MODES // UNROLL * UNROLL, MODES):
        mix(k, None)

    def synthesise(pair, carry):
        both = coefs[:, pl.ds(pair * 2 * STRIPS, 2 * STRIPS), :].astype(jnp.float32)
        for half in range(2):
            row = 2 * pair + half
            mixed = both[:, half * STRIPS : (half + 1) * STRIPS]
            mixed = mixed.reshape(COEFS * STRIPS, channels).astype(jnp.bfloat16)
            cells = pl.ds(lo - source_lo, hi - lo)
            centre = source[first + row + 1, cells]
            hidden = jnp.dot(backward[lo:hi], mixed, preferred_element_type=jnp.float32)
            hidden = hidden + jnp.dot(centre, skip[...], preferred_element_type=jnp.float32)
            wide = centre.astype(jnp.float32)
            laplacian = (
                source[first + row + 2, cells].astype(jnp.float32) + source[first + row, cells].astype(jnp.float32) - 2.0 * wide
            )
            hidden = hidden + diff * laplacian
            result = wide + gelu(hidden)
            if valid is not None:
                result = jnp.where(valid(row), result, 0.0)
            target[target_first + row] = result.astype(jnp.bfloat16)
        return carry

    for pair in range(pairs):
        synthesise(pair, None)


def kernel(
    group_rows, band_rows, grid_rows, count, lats,
    padded, spec_hbm, skip, diffusion, forward, forward_inner, backward,
    result,
    window, middle, final, coefs, spec, edges,
    spec_sems, own_sems, put_sems, y_send, y_recv, z_send, z_recv, lat_send, lat_recv, out_send, out_recv,
):
    index = lax.axis_index("lon")
    lat = lax.axis_index("lat")
    place = lax.rem(index, GROUP)
    base = index - place
    quarter = group_rows // CHUNKS
    length = STRIPS * HOP
    pieces = [
        (quarter, quarter + 4),
        (2 * quarter + 4, quarter),
        (0, quarter),
        (3 * quarter + 4, quarter),
    ]
    upward = lax.rem(index + GROUP, count)
    downward = lax.rem(index + count - GROUP, count)

    def xor(d):
        low = lax.rem(place, 2)
        high = place // 2
        low = 1 - low if d & 1 else low
        high = 1 - high if d & 2 else high
        return 2 * high + low

    def strip(at):
        return pl.ds(pl.multiple_of((at + 2) * HOP, HOP), HOP)

    def remote(source, target, send, recv, where):
        return pltpu.make_async_remote_copy(
            src_ref=source, dst_ref=target, send_sem=send, recv_sem=recv,
            device_id=where, device_id_type=pl.DeviceIdType.MESH,
        )

    def y_copy(n, d, receive):
        first, number = pieces[n]
        other = xor(d)
        owner = other if receive else place
        return remote(
            padded.at[pl.ds(other * group_rows + first, number)],
            window.at[pl.ds(first, number), strip(owner)],
            y_send.at[n, d], y_recv.at[n, d], {"lon": base + other},
        )

    def z_copy(n, side, receive):
        first, number = pieces[n]
        rows = pl.ds(first, number)
        if side == 0:
            source, target, where = 4 * HOP, 0, upward
        else:
            source, target, where = 2 * HOP, 6 * HOP, downward
        return remote(
            window.at[rows, pl.ds(source, 2 * HOP)],
            window.at[rows, pl.ds(target, 2 * HOP)],
            z_send.at[n, side], z_recv.at[n, side], {"lon": where},
        )

    def out_copy(chunk, d, receive):
        other = xor(d)
        owner = other if receive else place
        return remote(
            final.at[pl.ds(chunk * quarter, quarter), pl.ds(pl.multiple_of(other * HOP, HOP), HOP)],
            result.at[pl.ds(owner * group_rows + chunk * quarter, quarter)],
            out_send.at[chunk, d], out_recv.at[chunk, d], {"lon": base + other},
        )

    own = []
    for n in range(CHUNKS):
        first, number = pieces[n]
        for d in (2, 3, 1):
            y_copy(n, d, False).start()
        copy = pltpu.make_async_copy(
            padded.at[pl.ds(place * group_rows + first, number)],
            window.at[pl.ds(first, number), strip(place)],
            own_sems.at[n],
        )
        copy.start()
        own.append(copy)
    loads = []
    for layer in range(LAYERS):
        copy = pltpu.make_async_copy(spec_hbm.at[layer], spec.at[layer], spec_sems.at[layer])
        copy.start()
        loads.append(copy)

    def forward_piece(n):
        own[n].wait()
        for d in (1, 2, 3):
            y_copy(n, d, True).wait_recv()
        for side in range(2):
            z_copy(n, side, False).start()

    forward_piece(0)
    forward_piece(1)

    low_edge = jnp.logical_and(place == 0, lat > 0)
    high_edge = jnp.logical_and(place == GROUP - 1, lat < lats - 1)

    def to_before():
        return remote(
            window.at[pl.ds(2, 2)], edges.at[1], lat_send.at[0], lat_recv.at[1],
            {"lon": base + GROUP - 1, "lat": jnp.maximum(lat - 1, 0)},
        )

    def to_after():
        return remote(
            window.at[pl.ds(group_rows, 2)], edges.at[0], lat_send.at[1], lat_recv.at[0],
            {"lon": base, "lat": jnp.minimum(lat + 1, lats - 1)},
        )

    def run(chunk, between=None):
        start = chunk * quarter
        top = lat * band_rows + place * group_rows + start - 1

        def valid(row):
            at = top + row
            return jnp.logical_and(at >= 0, at < grid_rows)

        layer_rows(
            quarter + 2, start, window, 0, middle, 0, HOP, length - HOP, forward, backward,
            spec.at[0], skip.at[0], diffusion[0:1], coefs, valid,
        )
        if between is not None:
            between()
        layer_rows(
            quarter, 0, middle, HOP, final, start, 2 * HOP, length - 2 * HOP, forward_inner, backward,
            spec.at[1], skip.at[1], diffusion[1:2], coefs, None,
        )
        for d in (2, 3, 1):
            out_copy(chunk, d, False).start()
        put = pltpu.make_async_copy(
            final.at[pl.ds(start, quarter), pl.ds(pl.multiple_of(place * HOP, HOP), HOP)],
            result.at[pl.ds(place * group_rows + start, quarter)],
            put_sems.at[chunk],
        )
        put.start()
        return put

    def arrived(n):
        for side in range(2):
            z_copy(n, side, True).wait_recv()
            z_copy(n, side, False).wait_send()

    puts = []
    arrived(0)
    for copy in loads:
        copy.wait()
    puts.append(run(1, lambda: forward_piece(2)))
    forward_piece(3)
    arrived(1)
    puts.append(run(2))
    arrived(2)

    @pl.when(low_edge)
    def _():
        to_before().start()

    arrived(3)

    @pl.when(high_edge)
    def _():
        to_after().start()
        to_before().wait_recv()
        window[group_rows + 2 : group_rows + 4] = edges[1]

    puts.append(run(3))

    @pl.when(low_edge)
    def _():
        to_after().wait_recv()
        window[0:2] = edges[0]

    puts.append(run(0))

    for put in puts:
        put.wait()

    @pl.when(low_edge)
    def _():
        to_before().wait_send()

    @pl.when(high_edge)
    def _():
        to_after().wait_send()

    for n in range(CHUNKS):
        for d in (1, 2, 3):
            y_copy(n, d, False).wait_send()
            out_copy(n, d, False).wait_send()
    for n in range(CHUNKS):
        for d in (1, 2, 3):
            out_copy(n, d, True).wait_recv()


def local(grid_rows, fields, spec_weight, skip_weight, diffusion):
    band_rows, strip, channels = fields.shape
    group_rows = band_rows // GROUP
    quarter = group_rows // CHUNKS
    length = STRIPS * HOP
    forward, backward = banded_tables()
    consts = (jnp.asarray(forward), jnp.asarray(forward[:, HOP:-HOP]), jnp.asarray(backward))
    padded = jnp.pad(fields, ((2, 2), (0, 0), (0, 0)))
    anywhere = pl.BlockSpec(memory_space=pl.ANY)
    inside = pl.BlockSpec(memory_space=pltpu.VMEM)
    dma = pltpu.SemaphoreType.DMA
    return pl.pallas_call(
        functools.partial(
            kernel, group_rows, band_rows, grid_rows, lax.axis_size("lon"), lax.axis_size("lat")
        ),
        out_shape=jax.ShapeDtypeStruct(fields.shape, jnp.bfloat16),
        in_specs=[anywhere] * 2 + [inside] * 5,
        out_specs=anywhere,
        scratch_shapes=[
            pltpu.VMEM((group_rows + 4, length, channels), jnp.bfloat16),
            pltpu.VMEM((quarter + 2, length - 2 * HOP, channels), jnp.bfloat16),
            pltpu.VMEM((group_rows, length - 4 * HOP, channels), jnp.bfloat16),
            pltpu.VMEM((COEFS, (quarter + 2) * STRIPS, channels), jnp.bfloat16),
            pltpu.VMEM(spec_weight.shape, jnp.bfloat16),
            pltpu.VMEM((2, 2, length, channels), jnp.bfloat16),
            dma((LAYERS,)), dma((CHUNKS,)), dma((CHUNKS,)),
            dma((CHUNKS, GROUP)), dma((CHUNKS, GROUP)),
            dma((CHUNKS, 2)), dma((CHUNKS, 2)),
            dma((2,)), dma((2,)),
            dma((CHUNKS, GROUP)), dma((CHUNKS, GROUP)),
        ],
        compiler_params=pltpu.CompilerParams(
            vmem_limit_bytes=56 * 1024 * 1024, has_side_effects=True
        ),
    )(padded, spec_weight, skip_weight, diffusion, *consts)


def solution(mesh):
    in_specs = (P("lat", "lon", None), P(), P(), P())
    out_specs = P("lat", "lon", None)

    def whole(fields, spec_weight, skip_weight, diffusion):
        step = functools.partial(local, fields.shape[0])
        return jax.shard_map(step, mesh=mesh, in_specs=in_specs, out_specs=out_specs, check_vma=False)(
            fields, spec_weight, skip_weight, diffusion
        )

    return whole
```
